32 devices in a mesh: rows: 8 (over y, x, core), cols: 4 (over z).
Axes of the slice: x: 2, y: 2, z: 4, core: 2. Of those that a mesh axis runs over, the one named last changes fastest.
Arguments:
- memory: float32 [128, 262144], P('cols', 'rows'), may hold values from -3 to 3
- last_tick: int32 [262144], P('rows'), may hold values from 0 to 999
- slot_node: int32 [64, 256], P('rows'), may hold values from 0 to 262143, as said below
- slot_pair: int32 [64, 256], P('rows'), may hold values from 0 to 2047, as said below
- slot_tick: int32 [64, 256], P('rows'), may hold values from 1000 to 1999
- block_count: int32 [8, 8], P('rows'), may hold values from 0 to 256, as said below
- time_freq: float32 [128], replicated, may hold values from 0.002 to 0.1
- time_phase: float32 [128], replicated, may hold values from -3.140625 to 3.140625
- w_pair: bfloat16 [128, 2, 384], P('cols'), may hold values from -0.3125 to 0.3125
- w_time: bfloat16 [128, 384], P('cols'), may hold values from -0.3125 to 0.3125
- w_hidden: bfloat16 [128, 384], P('cols'), may hold values from -0.5 to 0.5
- bias_input: float32 [384], P('cols'), may hold values from -3 to 3
- bias_hidden: float32 [384], P('cols'), may hold values from -3 to 3
Outputs:
- new_memory: float32 [128, 262144], P('cols', 'rows')
The draws below stay inside these ranges and needn't reach their ends.
Inputs may be any that keep to these rules, and one draw needn't show every extreme that they name: `slot_node`: every slot of block b (live or not) names a node of owner b, from b * 32768 to (b + 1) * 32768 - 1. `slot_pair`: indexes the holder's 8 * 256 slots flattened block by block; the relation is symmetric without fixed points, and live slots pair with live slots. `block_count`: every count is even; in every draw one owner's block is full (256 live slots) from every holder.
All inputs are finite; a program needn't handle non-finite values.
Results may differ from the reference program's by a relative error of at most 0.0006.
Values may be sent and summed in bfloat16 or wider, within the bound.
A program may use at most 128 MiB of HBM per device.

```python
import math
import jax
import jax.numpy as jnp
from jax import lax

MEM = 128
TDIM = 128
NODE_DEV = 32768
CAP = 256
TICK_SPAN = 1000
NODES = 262144
N_ROWS = 8


def layout_all(key):
    base_key = jax.random.fold_in(key, 7)
    hot_key, count_key, node_key, order_key = jax.random.split(base_key, 4)
    hottest = jax.random.randint(hot_key, (), 0, N_ROWS)
    drawn = 2 * jax.random.randint(count_key, (N_ROWS, N_ROWS), CAP // 16, 5 * CAP // 32 + 1)
    counts = jnp.where(jnp.arange(N_ROWS)[None, :] == hottest, CAP, drawn).astype(jnp.int32)
    local = jax.random.randint(node_key, (N_ROWS, N_ROWS, CAP), 0, NODE_DEV)
    nodes = (jnp.arange(N_ROWS)[None, :, None] * NODE_DEV + local).astype(jnp.int32)
    span = N_ROWS * CAP
    filled = (jnp.arange(CAP)[None, None, :] < counts[:, :, None]).reshape(N_ROWS, span)
    ranks = jax.vmap(lambda k: jax.random.permutation(k, span))(jax.random.split(order_key, N_ROWS))
    score = jnp.where(filled, 0, span) + ranks
    order = jnp.argsort(score, axis=1, stable=True).astype(jnp.int32)
    flipped = jnp.arange(span) ^ 1

    def pair_row(row_order):
        return jnp.zeros((span,), jnp.int32).at[row_order].set(row_order[flipped])
    pairs = jax.vmap(pair_row)(order)
    return (counts, nodes.reshape(N_ROWS * N_ROWS, CAP), pairs.reshape(N_ROWS * N_ROWS, CAP))


def draw_block_count(key, part):
    return layout_all(key)[0]


def draw_slot_node(key, part):
    return layout_all(key)[1]


def draw_slot_pair(key, part):
    return layout_all(key)[2]


def set_ends(values, stream_key, low, high):
    longest = values.shape.index(max(values.shape))
    spots = []
    for shift in (0, 1):
        where = [jax.random.randint(jax.random.fold_in(stream_key, axis), (), 0, length) for axis, length in enumerate(values.shape)]
        where[longest] = (where[longest] + shift) % values.shape[longest]
        spots.append(tuple(where))
    return values.at[spots[0]].set(low).at[spots[1]].set(high)


def block_scale(rng, shape, pieces, low, largest):
    loudness = 1.0
    for position, shards_of in pieces:
        heights = jax.random.uniform(jax.random.fold_in(jax.random.fold_in(rng, 6), position), (shards_of,), jnp.float32, low / len(pieces), largest / len(pieces))
        loudness = loudness * jnp.repeat(jnp.exp(heights), shape[position] // shards_of).reshape((-1,) + (1,) * (len(shape) - 1 - position))
    return loudness


def centred(key, shape, scale, most, cuts=(), kind=jnp.bfloat16):
    level = block_scale(key, shape, cuts, -0.22, 0.18) if cuts else 1.0
    drawn = jax.random.normal(key, shape, jnp.float32) * scale * level
    return jnp.minimum(jnp.maximum(drawn, -most), most).astype(kind)


def setup_inputs(seed: int = 0) -> dict:
    keys = jax.random.split(jax.random.key(seed), 14)
    return {
        "memory": centred(keys[0], (MEM, NODES), 0.5, 3.0, ((0, 4), (1, 8)), jnp.float32),
        "last_tick": set_ends(jax.random.randint(keys[1], (NODES,), 0, TICK_SPAN), jax.random.fold_in(keys[1], 1), 0, TICK_SPAN - 1).astype(jnp.int32),
        "slot_node": draw_slot_node(jax.random.fold_in(keys[13], 71), 0),
        "slot_pair": draw_slot_pair(jax.random.fold_in(keys[13], 71), 0),
        "slot_tick": set_ends(jax.random.randint(keys[4], (N_ROWS * N_ROWS, CAP), TICK_SPAN, 2 * TICK_SPAN), jax.random.fold_in(keys[4], 1), TICK_SPAN, (2 * TICK_SPAN) - 1).astype(jnp.int32),
        "block_count": draw_block_count(jax.random.fold_in(keys[13], 71), 0),
        "time_freq": jnp.clip(jnp.exp(jax.random.uniform(keys[6], (TDIM,), jnp.float32, math.log(0.002), math.log(0.1))), 0.002, 0.1),
        "time_phase": jnp.clip(jax.random.uniform(keys[7], (TDIM,), jnp.float32, -3.140625, 3.140625), -3.140625, 3.140625),
        "w_pair": centred(keys[8], (MEM, 2, 3 * MEM), (2 * MEM + TDIM) ** -0.5, 0.3125, ((0, 4),)),
        "w_time": centred(keys[9], (TDIM, 3 * MEM), (2 * MEM + TDIM) ** -0.5, 0.3125, ((0, 4),)),
        "w_hidden": centred(keys[10], (MEM, 3 * MEM), MEM ** -0.5, 0.5, ((0, 4),)),
        "bias_input": centred(keys[11], (3 * MEM,), 0.5, 3.0, ((0, 4),), jnp.float32),
        "bias_hidden": centred(keys[12], (3 * MEM,), 0.5, 3.0, ((0, 4),), jnp.float32),
    }


def reference(memory, last_tick, slot_node, slot_pair, slot_tick, block_count, time_freq, time_phase, w_pair, w_time, w_hidden, bias_input, bias_hidden):
    width = memory.shape[0]
    slots = slot_node.reshape(N_ROWS, N_ROWS, CAP)
    flat_nodes = slot_node.reshape(N_ROWS, N_ROWS * CAP)
    partners = jnp.take_along_axis(flat_nodes, slot_pair.reshape(N_ROWS, N_ROWS * CAP), axis=1).reshape(N_ROWS, N_ROWS, CAP)
    ticks = slot_tick.reshape(N_ROWS, N_ROWS, CAP)
    filled = jnp.arange(CAP, dtype=jnp.int32)[None, None, :] < block_count[:, :, None]

    def owner_block(owner):
        nodes = slots[:, owner].reshape(-1)
        others = partners[:, owner].reshape(-1)
        live = filled[:, owner].reshape(-1)
        hidden = memory[:, nodes].T
        self_in = hidden.astype(jnp.bfloat16)
        partner_in = memory[:, others].T.astype(jnp.bfloat16)
        gaps = (ticks[:, owner].reshape(-1) - last_tick[nodes]).astype(jnp.float32)
        encoded = jnp.cos(gaps[:, None] * time_freq[None, :] + time_phase[None, :]).astype(jnp.bfloat16)
        gate_in = jnp.dot(self_in, w_pair[:, 0, :], preferred_element_type=jnp.float32)
        gate_in = gate_in + jnp.dot(partner_in, w_pair[:, 1, :], preferred_element_type=jnp.float32)
        gate_in = gate_in + jnp.dot(encoded, w_time, preferred_element_type=jnp.float32)
        gate_hid = jnp.dot(self_in, w_hidden, preferred_element_type=jnp.float32)
        local = jnp.where(live, nodes - owner * NODE_DEV, NODE_DEV).astype(jnp.int32)
        sums = jnp.zeros((NODE_DEV + 1, 3 * width), jnp.float32).at[local].add(gate_in)
        counts = jnp.zeros((NODE_DEV + 1,), jnp.float32).at[NODE_DEV].set(1.0).at[local].add(1.0)
        mean = sums[local] / counts[local][:, None]
        gx = (mean + bias_input[None, :]).reshape(-1, width, 3)
        gh = (gate_hid + bias_hidden[None, :]).reshape(-1, width, 3)
        reset = jax.nn.sigmoid(gx[:, :, 0] + gh[:, :, 0])
        keep = jax.nn.sigmoid(gx[:, :, 1] + gh[:, :, 1])
        cand = jnp.tanh(gx[:, :, 2] + reset * gh[:, :, 2])
        fresh = (1.0 - keep) * cand + keep * hidden
        block = lax.dynamic_slice_in_dim(memory, owner * NODE_DEV, NODE_DEV, 1)
        return block.at[:, local].set(fresh.T, mode="drop")

    result = lax.map(owner_block, jnp.arange(N_ROWS, dtype=jnp.int32))
    return jnp.transpose(result, (1, 0, 2)).reshape(width, N_ROWS * NODE_DEV)
```

```python
import functools

import jax
import jax.numpy as jnp
from jax import lax
from jax.experimental import pallas as pl
from jax.experimental.pallas import tpu as pltpu
from jax.sharding import PartitionSpec as P

MESH = pl.DeviceIdType.MESH
LANES = 128
VM = pl.BlockSpec(memory_space=pltpu.VMEM)
SM = pl.BlockSpec(memory_space=pltpu.SMEM)
ANY = pl.BlockSpec(memory_space=pl.ANY)


def greet(axis, n):
    barrier = pltpu.get_barrier_semaphore()
    me = lax.axis_index(axis)
    for k in range(1, n):
        pl.semaphore_signal(
            barrier, inc=1, device_id={axis: lax.rem(me + k, n)}, device_id_type=MESH
        )


def exchange(axis, n, src, dst, send, recv):
    me = lax.axis_index(axis)
    copies = []
    for k in range(1, n):
        peer = lax.rem(me + k, n)
        copies.append(
            pltpu.make_async_remote_copy(
                src_ref=src.at[peer],
                dst_ref=dst.at[me],
                send_sem=send.at[k],
                recv_sem=recv.at[k],
                device_id={axis: peer},
                device_id_type=MESH,
            )
        )
    for copy in copies:
        copy.start()
    return copies


def first_kernel(n, c, meta, w, meta_out, w_out, ssem, rsem, wssem, wrsem):
    greet("rows", n)
    greet("cols", c)
    pl.semaphore_wait(pltpu.get_barrier_semaphore(), n + c - 2)
    copies = exchange("rows", n, meta, meta_out, ssem, rsem)
    copies += exchange("cols", c, w, w_out, wssem, wrsem)
    row, col = lax.axis_index("rows"), lax.axis_index("cols")
    meta_out[row] = meta[row]
    w_out[col] = w[col]
    for copy in copies:
        copy.wait()


def reply_kernel(n, src, dst, ssem, rsem):
    greet("rows", n)
    pl.semaphore_wait(pltpu.get_barrier_semaphore(), n - 1)
    copies = exchange("rows", n, src, dst, ssem, rsem)
    row = lax.axis_index("rows")
    dst[row] = src[row]
    for copy in copies:
        copy.wait()


def spread_kernel(
    n, c, perm, own, self_all, part_all, own_sem, ssem, rsem, sls, slr, srs, srr, pls, plr, prs, prr
):
    row, col = lax.axis_index("rows"), lax.axis_index("cols")
    barrier = pltpu.get_barrier_semaphore()
    greet("rows", n)
    greet("cols", c)
    pl.semaphore_wait(barrier, n + c - 2)

    def hop(src, dst, send, recv, to):
        return pltpu.make_async_remote_copy(
            src_ref=src,
            dst_ref=dst,
            send_sem=send,
            recv_sem=recv,
            device_id={"cols": to},
            device_id_type=MESH,
        )

    first = pltpu.make_async_copy(perm.at[row], part_all.at[col, row], own_sem.at[0])
    first.start()
    copies = []
    for k in range(1, n):
        peer = lax.rem(row + k, n)
        copies.append(
            pltpu.make_async_remote_copy(
                src_ref=perm.at[peer],
                dst_ref=part_all.at[col, row],
                send_sem=ssem.at[k],
                recv_sem=rsem.at[k],
                device_id={"rows": peer},
                device_id_type=MESH,
            )
        )
    for copy in copies:
        copy.start()
    second = pltpu.make_async_copy(own, self_all.at[col], own_sem.at[1])
    second.start()

    def self_hop(source, t, right):
        sem_s, sem_r = (srs, srr) if right else (sls, slr)
        ref = self_all.at[source]
        src = own if t == 0 else ref
        return hop(src, ref, sem_s.at[t], sem_r.at[t], col + 1 if right else col - 1)

    def part_hop(source, place, t, k, right):
        sem_s, sem_r = (prs, prr) if right else (pls, plr)
        ref = part_all.at[source, place]
        return hop(ref, ref, sem_s.at[t, k], sem_r.at[t, k], col + 1 if right else col - 1)

    can = {True: lambda: col < c - 1, False: lambda: col > 0}
    for right in (True, False):

        @pl.when(can[right]())
        def _(right=right):
            self_hop(col, 0, right).start()

    first.wait()
    for k in range(n):
        place = lax.rem(row - k + n, n)
        if k:
            copies[k - 1].wait_recv()
        for right in (True, False):

            @pl.when(can[right]())
            def _(right=right, k=k, place=place):
                part_hop(col, place, 0, k, right).start()

    for t in range(1, c):
        for right in (True, False):
            source = col - t if right else col + t
            there = source >= 0 if right else source < c
            onward = jnp.logical_and(there, can[right]())

            @pl.when(there)
            def _(right=right, t=t, source=source):
                self_hop(source, t - 1, right).wait_recv()

            @pl.when(onward)
            def _(right=right, t=t, source=source):
                self_hop(source, t, right).start()

        for k in range(n):
            place = lax.rem(row - k + n, n)
            for right in (True, False):
                source = col - t if right else col + t
                there = source >= 0 if right else source < c
                onward = jnp.logical_and(there, can[right]())

                @pl.when(there)
                def _(right=right, t=t, source=source, k=k, place=place):
                    part_hop(source, place, t - 1, k, right).wait_recv()

                @pl.when(onward)
                def _(right=right, t=t, source=source, k=k, place=place):
                    part_hop(source, place, t, k, right).start()

    second.wait()
    for copy in copies:
        copy.wait_send()
    for t in range(c - 1):
        for right in (True, False):
            source = col - t if right else col + t
            there = source >= 0 if right else source < c
            onward = jnp.logical_and(there, can[right]())

            @pl.when(onward)
            def _(right=right, t=t, source=source):
                self_hop(source, t, right).wait_send()
                for k in range(n):
                    part_hop(source, lax.rem(row - k + n, n), t, k, right).wait_send()


def gather_kernel(ids, ticks, memory, last, own, own16, gaps):
    wp, node_rows = memory.shape
    cap = ids.shape[1]
    per = cap // LANES
    lane = lax.broadcasted_iota(jnp.int32, (wp, LANES), 1)
    lane1 = lax.broadcasted_iota(jnp.int32, (1, LANES), 1)

    def tile(i, _):
        block, half = i // per, lax.rem(i, per)

        def slot(j, carry):
            acc, tacc = carry
            node = jnp.minimum(ids[block, half * LANES + j], node_rows - 1)
            t = lax.shift_right_logical(node, 7)
            shift = lax.bitwise_and(j - lax.bitwise_and(node, LANES - 1), LANES - 1)
            x = memory[:, pl.ds(pl.multiple_of(t * LANES, LANES), LANES)]
            acc = jnp.where(lane == j, pltpu.roll(x, shift, 1), acc)
            y = last[pl.ds(t, 1), :]
            tacc = jnp.where(lane1 == j, pltpu.roll(y, shift, 1), tacc)
            return acc, tacc

        zero = (jnp.zeros((wp, LANES), jnp.float32), jnp.zeros((1, LANES), jnp.int32))
        acc, tacc = lax.fori_loop(0, LANES, slot, zero, unroll=16)
        own[:, pl.ds(pl.multiple_of(i * LANES, LANES), LANES)] = acc
        own16[block, :, pl.ds(pl.multiple_of(half * LANES, LANES), LANES)] = acc.astype(
            jnp.bfloat16
        )
        gaps[pl.ds(i, 1), :] = (ticks[pl.ds(i, 1), :] - tacc).astype(jnp.float32)
        return 0

    lax.fori_loop(0, ids.shape[0] * per, tile, 0)


def permute_kernel(held, pair, out, wide):
    n, wp, cap = held.shape
    per = cap // LANES
    tiles = n * per
    for k in range(tiles):
        wide[k] = held[k // per, :, (k % per) * LANES : (k % per + 1) * LANES].astype(jnp.float32)

    def tile(i, _):
        p = pair[pl.ds(i, 1), :]
        where = jnp.broadcast_to(lax.shift_right_logical(p, 7), (8, LANES))
        lane = jnp.broadcast_to(lax.bitwise_and(p, LANES - 1), (8, LANES))
        parts = [jnp.zeros((8, LANES), jnp.float32) for _ in range(wp // 8)]
        for k in range(tiles):
            hit = where == k
            for r in range(wp // 8):
                got = jnp.take_along_axis(wide[k, r * 8 : (r + 1) * 8, :], lane, axis=1)
                parts[r] = jnp.where(hit, got, parts[r])
        whole = jnp.concatenate(parts, axis=0).astype(jnp.bfloat16)
        block, half = i // per, lax.rem(i, per)
        out[block, :, pl.ds(pl.multiple_of(half * LANES, LANES), LANES)] = whole
        return 0

    lax.fori_loop(0, tiles, tile, 0)


def update_kernel(
    ids,
    idrow,
    gaps,
    w,
    bias,
    timing,
    self_all,
    part_all,
    own,
    memory,
    out,
    sem,
    gate_parts,
    gate_hid,
    equal,
    columns,
    fresh,
):
    c, n, wp, cap = self_all.shape
    node_rows = memory.shape[1]
    per = cap // LANES
    tiles = n * per
    g3 = 3 * wp
    load = pltpu.make_async_copy(memory, out, sem)
    load.start()

    from_col = lax.broadcasted_iota(jnp.int32, (g3, g3), 0)
    to_col = lax.broadcasted_iota(jnp.int32, (g3, g3), 1)
    gate, feature = to_col // wp, lax.rem(to_col, wp)
    order = (from_col == 3 * feature + gate).astype(jnp.float32).astype(jnp.bfloat16)

    def weights(kind):
        rows = w[:, kind].reshape(c * wp, g3)
        return jnp.dot(rows, order, preferred_element_type=jnp.float32).astype(jnp.bfloat16)

    w_self, w_part, w_time, w_hid = (weights(k) for k in range(4))
    over_in = (((0,), (0,)), ((), ()))

    def mm(a, b):
        return lax.dot_general(a, b, over_in, preferred_element_type=jnp.float32)

    gate_parts[2 * g3 :, :] = jnp.ones((gate_parts.shape[0] - 2 * g3, n * cap), jnp.bfloat16)

    def chunk(b, _):
        lanes = pl.ds(pl.multiple_of(b * cap, cap), cap)
        xs = self_all[:, b].reshape(c * wp, cap)
        xp = part_all[:, b].reshape(c * wp, cap)
        gap = jnp.concatenate([gaps[pl.ds(b * per + h, 1), :] for h in range(per)], axis=1)
        encoded = jnp.cos(gap * timing[:, 0:1] + timing[:, 1:2]).astype(jnp.bfloat16)
        gi = mm(w_self, xs) + mm(w_part, xp) + mm(w_time, encoded)
        gate_hid[:, lanes] = mm(w_hid, xs) + bias[:, 1:2]
        high = gi.astype(jnp.bfloat16)
        gate_parts[0:g3, lanes] = high
        gate_parts[g3 : 2 * g3, lanes] = (gi - high.astype(jnp.float32)).astype(jnp.bfloat16)
        return 0

    lax.fori_loop(0, n, chunk, 0)

    def column(i, _):
        row = jnp.broadcast_to(idrow[pl.ds(i, 1), :], (LANES, LANES))
        columns[pl.ds(pl.multiple_of(i * LANES, LANES), LANES), :] = row.T
        return 0

    lax.fori_loop(0, tiles, column, 0)

    def means(b, _):
        lanes = pl.ds(pl.multiple_of(b * cap, cap), cap)
        for h in range(per):
            row = idrow[pl.ds(b * per + h, 1), :]
            same = (columns[...] == row).astype(jnp.float32).astype(jnp.bfloat16)
            equal[:, h * LANES : (h + 1) * LANES] = same
        sums = jnp.dot(gate_parts[...], equal[...], preferred_element_type=jnp.float32)
        mean = (sums[0:g3] + sums[g3 : 2 * g3]) / sums[2 * g3 : 2 * g3 + 1]
        gx = mean + bias[:, 0:1]
        gh = gate_hid[:, lanes]
        reset = jax.nn.sigmoid(gx[0:wp] + gh[0:wp])
        keep = jax.nn.sigmoid(gx[wp : 2 * wp] + gh[wp : 2 * wp])
        cand = jnp.tanh(gx[2 * wp :] + reset * gh[2 * wp :])
        fresh[:, lanes] = (1.0 - keep) * cand + keep * own[:, lanes]
        return 0

    lax.fori_loop(0, n, means, 0)
    load.wait()
    lane = lax.broadcasted_iota(jnp.int32, (wp, LANES), 1)

    def tile(i, _):
        block, half = i // per, lax.rem(i, per)
        value = fresh[:, pl.ds(pl.multiple_of(i * LANES, LANES), LANES)]

        def slot(j, _):
            node = ids[block, half * LANES + j]
            safe = jnp.minimum(node, node_rows - 1)
            t = lax.shift_right_logical(safe, 7)
            place = lax.bitwise_and(node, LANES - 1)
            shift = lax.bitwise_and(place - j, LANES - 1)
            place = jnp.where(node < node_rows, place, LANES)
            pltpu.store(
                out.at[:, pl.ds(pl.multiple_of(t * LANES, LANES), LANES)],
                pltpu.roll(value, shift, 1),
                mask=lane == place,
            )
            return 0

        lax.fori_loop(0, LANES, slot, 0, unroll=16)
        return 0

    lax.fori_loop(0, tiles, tile, 0)


def comm(collective):
    return pltpu.CompilerParams(collective_id=collective, has_side_effects=True)


def dma(*shape):
    return pltpu.SemaphoreType.DMA(shape)


def local(
    n,
    c,
    memory,
    last_tick,
    slot_node,
    slot_pair,
    slot_tick,
    block_count,
    time_freq,
    time_phase,
    w_pair,
    w_time,
    w_hidden,
    bias_input,
    bias_hidden,
):
    wp, node_rows = memory.shape
    cap = slot_node.shape[1]
    total = n * cap
    tiles = total // LANES
    g3 = 3 * wp
    f32, i32, b16 = jnp.float32, jnp.int32, jnp.bfloat16
    shape = jax.ShapeDtypeStruct
    block_iota = lax.broadcasted_iota(i32, (n, cap), 0)
    slot_iota = lax.broadcasted_iota(i32, (n, cap), 1)
    filled = slot_iota < block_count.reshape(n, 1)
    local_ids = jnp.where(filled, slot_node - block_iota * node_rows, node_rows)
    meta = jnp.stack([local_ids, slot_tick], axis=1)
    w = jnp.stack([w_pair[:, 0], w_pair[:, 1], w_time, w_hidden], axis=0)
    w = w.reshape(4, wp, c, g3).transpose(2, 0, 1, 3)
    meta, w = pl.pallas_call(
        functools.partial(first_kernel, n, c),
        out_shape=(shape(meta.shape, i32), shape(w.shape, b16)),
        in_specs=[VM, VM],
        out_specs=(VM, VM),
        scratch_shapes=[dma(n), dma(n), dma(c), dma(c)],
        compiler_params=comm(1),
        name="first",
    )(meta, w)
    ids, ticks = meta[:, 0], meta[:, 1].reshape(tiles, LANES)
    own, own16, gaps = pl.pallas_call(
        gather_kernel,
        out_shape=(shape((wp, total), f32), shape((n, wp, cap), b16), shape((tiles, LANES), f32)),
        in_specs=[SM, VM, VM, VM],
        out_specs=(VM, VM, VM),
        name="gather",
    )(ids, ticks, memory, last_tick.reshape(node_rows // LANES, LANES))
    held = pl.pallas_call(
        functools.partial(reply_kernel, n),
        out_shape=shape((n, wp, cap), b16),
        in_specs=[VM],
        out_specs=VM,
        scratch_shapes=[dma(n), dma(n)],
        compiler_params=comm(2),
        name="reply",
    )(own16)
    perm = pl.pallas_call(
        permute_kernel,
        out_shape=shape((n, wp, cap), b16),
        in_specs=[VM, VM],
        out_specs=VM,
        scratch_shapes=[pltpu.VMEM((tiles, wp, LANES), f32)],
        name="permute",
    )(held, slot_pair.reshape(tiles, LANES))
    self_all, part_all = pl.pallas_call(
        functools.partial(spread_kernel, n, c),
        out_shape=(shape((c, n, wp, cap), b16), shape((c, n, wp, cap), b16)),
        in_specs=[VM, VM],
        out_specs=(VM, VM),
        scratch_shapes=[dma(2), dma(n), dma(n)] + [dma(c)] * 4 + [dma(c, n)] * 4,
        compiler_params=comm(3),
        name="spread",
    )(perm, own16)
    bias = jnp.stack(
        [bias_input.reshape(wp, 3).T.reshape(g3), bias_hidden.reshape(wp, 3).T.reshape(g3)], axis=1
    )
    timing = jnp.stack([time_freq, time_phase], axis=1)
    extra = 16
    return pl.pallas_call(
        update_kernel,
        out_shape=shape((wp, node_rows), f32),
        in_specs=[SM] + [VM] * 8 + [ANY],
        out_specs=VM,
        scratch_shapes=[
            pltpu.SemaphoreType.DMA,
            pltpu.VMEM((2 * g3 + extra, total), b16),
            pltpu.VMEM((g3, total), f32),
            pltpu.VMEM((total, cap), b16),
            pltpu.VMEM((total, LANES), f32),
            pltpu.VMEM((wp, total), f32),
        ],
        name="update",
    )(
        ids,
        ids.reshape(tiles, LANES).astype(f32),
        gaps,
        w,
        bias,
        timing,
        self_all,
        part_all,
        own,
        memory,
    )


def solution(mesh):
    placed = (
        P("cols", "rows"),
        P("rows"),
        P("rows", None),
        P("rows", None),
        P("rows", None),
        P("rows", None),
        P(),
        P(),
        P("cols", None, None),
        P("cols", None),
        P("cols", None),
        P("cols"),
        P("cols"),
    )
    return jax.shard_map(
        functools.partial(local, mesh.shape["rows"], mesh.shape["cols"]),
        mesh=mesh,
        in_specs=placed,
        out_specs=P("cols", "rows"),
        check_vma=False,
    )
```

```python
import functools

import jax
import jax.numpy as jnp
from jax import lax
from jax.experimental import pallas as pl
from jax.experimental.pallas import tpu as pltpu
from jax.sharding import PartitionSpec as P

MESH = pl.DeviceIdType.MESH
LANES = 128
VM = pl.BlockSpec(memory_space=pltpu.VMEM)
SM = pl.BlockSpec(memory_space=pltpu.SMEM)
ANY = pl.BlockSpec(memory_space=pl.ANY)


def greet(axis, n):
    barrier = pltpu.get_barrier_semaphore()
    me = lax.axis_index(axis)
    for k in range(1, n):
        pl.semaphore_signal(
            barrier, inc=1, device_id={axis: lax.rem(me + k, n)}, device_id_type=MESH
        )


def exchange(axis, n, src, dst, send, recv):
    me = lax.axis_index(axis)
    copies = []
    for k in range(1, n):
        peer = lax.rem(me + k, n)
        copies.append(
            pltpu.make_async_remote_copy(
                src_ref=src.at[peer],
                dst_ref=dst.at[me],
                send_sem=send.at[k],
                recv_sem=recv.at[k],
                device_id={axis: peer},
                device_id_type=MESH,
            )
        )
    for copy in copies:
        copy.start()
    return copies


def first_kernel(n, c, meta, w, meta_out, w_out, ssem, rsem, wssem, wrsem):
    greet("rows", n)
    greet("cols", c)
    pl.semaphore_wait(pltpu.get_barrier_semaphore(), n + c - 2)
    copies = exchange("rows", n, meta, meta_out, ssem, rsem)
    copies += exchange("cols", c, w, w_out, wssem, wrsem)
    row, col = lax.axis_index("rows"), lax.axis_index("cols")
    meta_out[row] = meta[row]
    w_out[col] = w[col]
    for copy in copies:
        copy.wait()


def chain(c, block, first, places, sems):
    col = lax.axis_index("cols")
    n = len(places)
    ways = (True, False)

    def hop(source, t, k, right):
        send, recv = sems[0:2] if right else sems[2:4]
        ref = block(source, places[k])
        return pltpu.make_async_remote_copy(
            src_ref=first(k) if t == 0 else ref,
            dst_ref=ref,
            send_sem=send.at[t, k],
            recv_sem=recv.at[t, k],
            device_id={"cols": col + 1 if right else col - 1},
            device_id_type=MESH,
        )

    def goes(right):
        return col < c - 1 if right else col > 0

    def where_from(t, right):
        source = col - t if right else col + t
        there = source >= 0 if right else source < c
        return source, there

    def begin(k):
        for right in ways:

            @pl.when(goes(right))
            def _(right=right):
                hop(col, 0, k, right).start()

    def rest():
        for t in range(1, c):
            for k in range(n):
                for right in ways:
                    source, there = where_from(t, right)

                    @pl.when(there)
                    def _(right=right, source=source, t=t, k=k):
                        hop(source, t - 1, k, right).wait_recv()

                    @pl.when(jnp.logical_and(there, goes(right)))
                    def _(right=right, source=source, t=t, k=k):
                        hop(source, t, k, right).start()

        for t in range(c - 1):
            for right in ways:
                source, there = where_from(t, right)

                @pl.when(jnp.logical_and(there, goes(right)))
                def _(right=right, source=source, t=t):
                    for k in range(n):
                        hop(source, t, k, right).wait_send()

    return begin, rest


def reply_kernel(n, c, src, dst, self_all, ssem, rsem, *sems):
    greet("rows", n)
    greet("cols", c)
    pl.semaphore_wait(pltpu.get_barrier_semaphore(), n + c - 2)
    copies = exchange("rows", n, src, dst, ssem, rsem)
    begin, rest = chain(
        c, lambda source, k: self_all.at[source, k], lambda k: src.at[k], list(range(n)), sems
    )
    for k in range(n):
        begin(k)
    row, col = lax.axis_index("rows"), lax.axis_index("cols")
    dst[row] = src[row]
    self_all[col] = src[...]
    rest()
    for copy in copies:
        copy.wait()


def spread_kernel(n, c, perm, part_all, ssem, rsem, *sems):
    row, col = lax.axis_index("rows"), lax.axis_index("cols")
    greet("rows", n)
    greet("cols", c)
    pl.semaphore_wait(pltpu.get_barrier_semaphore(), n + c - 2)
    copies = []
    for k in range(1, n):
        peer = lax.rem(row + k, n)
        copies.append(
            pltpu.make_async_remote_copy(
                src_ref=perm.at[peer],
                dst_ref=part_all.at[col, row],
                send_sem=ssem.at[k],
                recv_sem=rsem.at[k],
                device_id={"rows": peer},
                device_id_type=MESH,
            )
        )
    for copy in copies:
        copy.start()
    places = [lax.rem(row - k + n, n) for k in range(n)]
    begin, rest = chain(
        c,
        lambda source, place: part_all.at[source, place],
        lambda k: part_all.at[col, places[k]] if k else perm.at[row],
        places,
        sems,
    )
    begin(0)
    part_all[col, row] = perm[row]
    for k in range(1, n):
        copies[k - 1].wait_recv()
        begin(k)
    rest()
    for copy in copies:
        copy.wait_send()


def prepare_kernel(nodes, ticks, counts, w_pair, w_time, w_hid, meta, w, node_rows):
    n, cap = nodes.shape
    c, _, _, g3 = w.shape
    lane = lax.broadcasted_iota(jnp.int32, (1, cap), 1)
    for b in range(n):
        mine = nodes[b : b + 1, :] - b * node_rows
        meta[b, 0:1, :] = jnp.where(lane < counts[0, b], mine, node_rows)
        meta[b, 1:2, :] = ticks[b : b + 1, :]
    width = c * g3
    kinds = (w_pair[:, 0:width], w_pair[:, width : 2 * width], w_time[...], w_hid[...])
    for k, kind in enumerate(kinds):
        for p in range(c):
            w[p, k] = kind[:, p * g3 : (p + 1) * g3]


def load_rows(wp, node_rows, pieces, memory, flat, rows, sems):
    groups = LANES // wp
    step = node_rows // pieces
    copies = []
    for i in range(pieces):
        part = pl.ds(i * step, step)
        copies.append(pltpu.make_async_copy(memory.at[:, part], flat.at[:, part], sems.at[i]))
    for copy in copies:
        copy.start()
    per_piece = step // (groups * LANES)

    def turn(q, _):
        tiles = [
            flat[:, pl.ds(pl.multiple_of((q * groups + k) * LANES, LANES), LANES)]
            for k in range(groups)
        ]
        rows[pl.ds(pl.multiple_of(q * LANES, LANES), LANES), :] = jnp.concatenate(tiles, 0).T
        return 0

    def finish():
        for i, copy in enumerate(copies):
            copy.wait()
            lax.fori_loop(i * per_piece, (i + 1) * per_piece, turn, 0, unroll=4)

    return finish


def row_of(node, groups):
    high = lax.shift_right_logical(node, 7 + groups.bit_length() - 1)
    return high * LANES + lax.bitwise_and(node, LANES - 1)


def gather_kernel(ids, meta, last, memory, own, own16, gaps, flat, rows, picked, tpicked, sems):
    wp, node_rows = memory.shape
    n, _, cap = meta.shape
    per = cap // LANES
    groups = LANES // wp
    finish = load_rows(wp, node_rows, sems.shape[0], memory, flat, rows, sems)
    finish()
    down = lax.broadcasted_iota(jnp.int32, (LANES, LANES), 0)

    def tile(i, _):
        block, half = i // per, lax.rem(i, per)
        lanes = pl.ds(pl.multiple_of(half * LANES, LANES), LANES)

        def slot(j, _):
            node = jnp.minimum(ids[block, 0, half * LANES + j], node_rows - 1)
            picked[pl.ds(j, 1), :] = rows[pl.ds(row_of(node, groups), 1), :]
            tpicked[pl.ds(j, 1), :] = last[pl.ds(lax.shift_right_logical(node, 7), 1), :]
            return 0

        lax.fori_loop(0, LANES, slot, 0, unroll=16)
        node = jnp.minimum(meta[block, 0:1, lanes], node_rows - 1)
        group = lax.bitwise_and(lax.shift_right_logical(node, 7), groups - 1)
        turned = picked[...].T
        mine = turned[0:wp]
        for k in range(1, groups):
            mine = jnp.where(group == k, turned[k * wp : (k + 1) * wp], mine)
        own[:, pl.ds(pl.multiple_of(i * LANES, LANES), LANES)] = mine
        own16[block, :, lanes] = mine.astype(jnp.bfloat16)
        old = tpicked[...].astype(jnp.float32).T
        old = jnp.where(down == lax.bitwise_and(node, LANES - 1), old, 0.0)
        old = jnp.sum(old, axis=0, keepdims=True)
        gaps[pl.ds(i, 1), :] = meta[block, 1:2, lanes].astype(jnp.float32) - old
        return 0

    lax.fori_loop(0, n * per, tile, 0)


def permute_kernel(held, pair, out, wide, flat):
    n, wp, cap = held.shape
    per = cap // LANES
    tiles = n * per
    for k in range(tiles):
        half = slice((k % per) * LANES, (k % per + 1) * LANES)
        flat[k : k + 1, :] = pair[k // per : k // per + 1, half]
        wide[k] = held[k // per, :, (k % per) * LANES : (k % per + 1) * LANES].astype(jnp.float32)

    def tile(block, half):
        p = flat[pl.ds(block * per + half, 1), :]
        where = jnp.broadcast_to(lax.shift_right_logical(p, 7), (8, LANES))
        lane = jnp.broadcast_to(lax.bitwise_and(p, LANES - 1), (8, LANES))
        parts = [jnp.zeros((8, LANES), jnp.float32) for _ in range(wp // 8)]
        for k in range(tiles):
            hit = where == k
            for r in range(wp // 8):
                got = jnp.take_along_axis(wide[k, r * 8 : (r + 1) * 8, :], lane, axis=1)
                parts[r] = jnp.where(hit, got, parts[r])
        whole = jnp.concatenate(parts, axis=0).astype(jnp.bfloat16)
        out[block, :, half * LANES : (half + 1) * LANES] = whole

    def both(block, _):
        for half in range(per):
            tile(block, half)
        return 0

    lax.fori_loop(0, n, both, 0)


def update_kernel(
    ids,
    meta,
    gaps,
    w,
    bias_in,
    bias_hid,
    freq,
    phase,
    self_all,
    part_all,
    own,
    memory,
    out,
    sems,
    out_sems,
    flat,
    rows,
    turned,
    gate_parts,
    gate_hid,
    equal,
    columns,
    fresh,
):
    c, n, wp, cap = self_all.shape
    node_rows = memory.shape[1]
    per = cap // LANES
    tiles = n * per
    g3 = 3 * wp
    groups = LANES // wp
    pieces = sems.shape[0]
    finish = load_rows(wp, node_rows, pieces, memory, flat, rows, sems)

    from_col = lax.broadcasted_iota(jnp.int32, (g3, g3), 0)
    to_col = lax.broadcasted_iota(jnp.int32, (g3, g3), 1)
    gate, feature = to_col // wp, lax.rem(to_col, wp)
    order = (from_col == 3 * feature + gate).astype(jnp.float32).astype(jnp.bfloat16)

    to_row = lax.broadcasted_iota(jnp.int32, (g3, g3), 0)
    hit = lax.broadcasted_iota(jnp.int32, (g3, g3), 1) == 3 * lax.rem(to_row, wp) + to_row // wp
    bias_x, bias_h = (
        jnp.sum(jnp.where(hit, ref[...], 0.0), axis=1, keepdims=True) for ref in (bias_in, bias_hid)
    )
    wide = (freq.shape[1],) * 2
    same_place = lax.broadcasted_iota(jnp.int32, wide, 0) == lax.broadcasted_iota(jnp.int32, wide, 1)
    rate, shift_by = (
        jnp.sum(jnp.where(same_place, ref[...], 0.0), axis=1, keepdims=True) for ref in (freq, phase)
    )

    def weights(kind):
        rows = w[:, kind].reshape(c * wp, g3)
        return jnp.dot(rows, order, preferred_element_type=jnp.float32).astype(jnp.bfloat16)

    w_self, w_part, w_time, w_hid = (weights(k) for k in range(4))
    over_in = (((0,), (0,)), ((), ()))

    def mm(a, b):
        return lax.dot_general(a, b, over_in, preferred_element_type=jnp.float32)

    gate_parts[2 * g3 :, :] = jnp.ones((gate_parts.shape[0] - 2 * g3, n * cap), jnp.bfloat16)

    def chunk(b, _):
        lanes = pl.ds(pl.multiple_of(b * cap, cap), cap)
        xs = self_all[:, b].reshape(c * wp, cap)
        xp = part_all[:, b].reshape(c * wp, cap)
        gap = jnp.concatenate([gaps[pl.ds(b * per + h, 1), :] for h in range(per)], axis=1)
        encoded = jnp.cos(gap * rate + shift_by).astype(jnp.bfloat16)
        gi = mm(w_self, xs) + mm(w_part, xp) + mm(w_time, encoded)
        gate_hid[:, lanes] = mm(w_hid, xs) + bias_h
        high = gi.astype(jnp.bfloat16)
        gate_parts[0:g3, lanes] = high
        gate_parts[g3 : 2 * g3, lanes] = (gi - high.astype(jnp.float32)).astype(jnp.bfloat16)
        return 0

    lax.fori_loop(0, n, chunk, 0)

    def column(i, _):
        lanes = pl.ds(pl.multiple_of(lax.rem(i, per) * LANES, LANES), LANES)
        row = jnp.broadcast_to(meta[i // per, 0:1, lanes].astype(jnp.float32), (LANES, LANES))
        columns[pl.ds(pl.multiple_of(i * LANES, LANES), LANES), :] = row.T
        return 0

    lax.fori_loop(0, tiles, column, 0)

    def means(b, _):
        lanes = pl.ds(pl.multiple_of(b * cap, cap), cap)
        for h in range(per):
            row = meta[b, 0:1, h * LANES : (h + 1) * LANES].astype(jnp.float32)
            same = (columns[...] == row).astype(jnp.float32).astype(jnp.bfloat16)
            equal[:, h * LANES : (h + 1) * LANES] = same
        sums = jnp.dot(gate_parts[...], equal[...], preferred_element_type=jnp.float32)
        mean = (sums[0:g3] + sums[g3 : 2 * g3]) / sums[2 * g3 : 2 * g3 + 1]
        gx = mean + bias_x
        gh = gate_hid[:, lanes]
        reset = jax.nn.sigmoid(gx[0:wp] + gh[0:wp])
        keep = jax.nn.sigmoid(gx[wp : 2 * wp] + gh[wp : 2 * wp])
        cand = jnp.tanh(gx[2 * wp :] + reset * gh[2 * wp :])
        fresh[:, lanes] = (1.0 - keep) * cand + keep * own[:, lanes]
        return 0

    lax.fori_loop(0, n, means, 0)
    finish()
    group_of = lax.broadcasted_iota(jnp.int32, (1, LANES), 1) // wp

    def tile(i, _):
        block, half = i // per, lax.rem(i, per)
        value = fresh[:, pl.ds(pl.multiple_of(i * LANES, LANES), LANES)]
        turned[...] = jnp.concatenate([value] * groups, axis=0).T

        def slot(j, _):
            node = ids[block, 0, half * LANES + j]
            safe = jnp.minimum(node, node_rows - 1)
            group = lax.bitwise_and(lax.shift_right_logical(safe, 7), groups - 1)
            group = jnp.where(node < node_rows, group, groups)
            pltpu.store(
                rows.at[pl.ds(row_of(safe, groups), 1), :],
                turned[pl.ds(j, 1), :],
                mask=group_of == group,
            )
            return 0

        lax.fori_loop(0, LANES, slot, 0, unroll=16)
        return 0

    lax.fori_loop(0, tiles, tile, 0)
    step = node_rows // pieces
    per_piece = step // (groups * LANES)

    def back(q, _):
        x = rows[pl.ds(pl.multiple_of(q * LANES, LANES), LANES), :].T
        for k in range(groups):
            lanes = pl.ds(pl.multiple_of((q * groups + k) * LANES, LANES), LANES)
            flat[:, lanes] = x[k * wp : (k + 1) * wp]
        return 0

    copies = []
    for i in range(pieces):
        lax.fori_loop(i * per_piece, (i + 1) * per_piece, back, 0, unroll=4)
        part = pl.ds(i * step, step)
        copies.append(pltpu.make_async_copy(flat.at[:, part], out.at[:, part], out_sems.at[i]))
        copies[-1].start()
    for copy in copies:
        copy.wait()


def comm(collective):
    return pltpu.CompilerParams(collective_id=collective, has_side_effects=True)


def dma(*shape):
    return pltpu.SemaphoreType.DMA(shape)


def local(
    n,
    c,
    memory,
    last_tick,
    slot_node,
    slot_pair,
    slot_tick,
    block_count,
    time_freq,
    time_phase,
    w_pair,
    w_time,
    w_hidden,
    bias_input,
    bias_hidden,
):
    wp, node_rows = memory.shape
    cap = slot_node.shape[1]
    total = n * cap
    tiles = total // LANES
    g3 = 3 * wp
    f32, i32, b16 = jnp.float32, jnp.int32, jnp.bfloat16
    shape = jax.ShapeDtypeStruct
    pieces = 8
    sent = (shape((n, 2, cap), i32), shape((c, 4, wp, g3), b16))
    meta, w = pl.pallas_call(
        lambda *refs: prepare_kernel(*refs, node_rows),
        out_shape=sent,
        in_specs=[VM, VM, SM, VM, VM, VM],
        out_specs=(VM, VM),
        name="prepare",
    )(slot_node, slot_tick, block_count, w_pair.reshape(wp, 2 * c * g3), w_time, w_hidden)
    meta, w = pl.pallas_call(
        functools.partial(first_kernel, n, c),
        out_shape=(shape(meta.shape, i32), shape(w.shape, b16)),
        in_specs=[VM, VM],
        out_specs=(VM, VM),
        scratch_shapes=[dma(n), dma(n), dma(c), dma(c)],
        compiler_params=comm(1),
        name="first",
    )(meta, w)
    own, own16, gaps = pl.pallas_call(
        gather_kernel,
        out_shape=(shape((wp, total), f32), shape((n, wp, cap), b16), shape((tiles, LANES), f32)),
        in_specs=[SM, VM, VM, ANY],
        out_specs=(VM, VM, VM),
        scratch_shapes=[
            pltpu.VMEM((wp, node_rows), f32),
            pltpu.VMEM((node_rows * wp // LANES, LANES), f32),
            pltpu.VMEM((LANES, LANES), f32),
            pltpu.VMEM((LANES, LANES), i32),
            dma(pieces),
        ],
        name="gather",
    )(meta, meta, last_tick.reshape(node_rows // LANES, LANES), memory)
    everyone = shape((c, n, wp, cap), b16)
    held, self_all = pl.pallas_call(
        functools.partial(reply_kernel, n, c),
        out_shape=(shape((n, wp, cap), b16), everyone),
        in_specs=[VM],
        out_specs=(VM, VM),
        scratch_shapes=[dma(n), dma(n)] + [dma(c, n)] * 4,
        compiler_params=comm(2),
        name="reply",
    )(own16)
    perm = pl.pallas_call(
        permute_kernel,
        out_shape=shape((n, wp, cap), b16),
        in_specs=[VM, VM],
        out_specs=VM,
        scratch_shapes=[pltpu.VMEM((tiles, wp, LANES), f32), pltpu.VMEM((tiles, LANES), i32)],
        name="permute",
    )(held, slot_pair)
    part_all = pl.pallas_call(
        functools.partial(spread_kernel, n, c),
        out_shape=everyone,
        in_specs=[VM],
        out_specs=VM,
        scratch_shapes=[dma(n), dma(n)] + [dma(c, n)] * 4,
        compiler_params=comm(3),
        name="spread",
    )(perm)
    extra = 16
    return pl.pallas_call(
        update_kernel,
        out_shape=shape((wp, node_rows), f32),
        in_specs=[SM] + [VM] * 10 + [ANY],
        out_specs=ANY,
        scratch_shapes=[
            dma(pieces),
            dma(pieces),
            pltpu.VMEM((wp, node_rows), f32),
            pltpu.VMEM((node_rows * wp // LANES, LANES), f32),
            pltpu.VMEM((LANES, LANES), f32),
            pltpu.VMEM((2 * g3 + extra, total), b16),
            pltpu.VMEM((g3, total), f32),
            pltpu.VMEM((total, cap), b16),
            pltpu.VMEM((total, LANES), f32),
            pltpu.VMEM((wp, total), f32),
        ],
        name="update",
    )(
        meta,
        meta,
        gaps,
        w,
        bias_input.reshape(1, g3),
        bias_hidden.reshape(1, g3),
        time_freq.reshape(1, -1),
        time_phase.reshape(1, -1),
        self_all,
        part_all,
        own,
        memory,
    )


def solution(mesh):
    placed = (
        P("cols", "rows"),
        P("rows"),
        P("rows", None),
        P("rows", None),
        P("rows", None),
        P("rows", None),
        P(),
        P(),
        P("cols", None, None),
        P("cols", None),
        P("cols", None),
        P("cols"),
        P("cols"),
    )
    return jax.shard_map(
        functools.partial(local, mesh.shape["rows"], mesh.shape["cols"]),
        mesh=mesh,
        in_specs=placed,
        out_specs=P("cols", "rows"),
        check_vma=False,
    )
```
